32 devices in a mesh: tm: 4 (over z), batch: 4 (over x, core), width: 2 (over y).
Axes of the slice: x: 2, y: 2, z: 4, core: 2. Of those that a mesh axis runs over, the one named last changes fastest.
Arguments:
- moves: int32 [8, 1024], P('batch', 'tm'), may hold values from 0 to 361
- lengths: int32 [8], P('batch'), may hold values from 1 to 1024
- outcomes: int32 [8], P('batch'), may hold values from -1 to 1
- embedded: bfloat16 [8, 1024, 2048], P('batch', 'tm', 'width'), may hold values from -6 to 6
- w_branches: bfloat16 [4, 2048, 2048], P(None, ('tm', 'batch'), 'width'), may hold values from -0.125 to 0.125
- conv_w: float32 [4, 2048], P(None, 'width'), may hold values from -3 to 3
- gate_bias: float32 [2, 2048], P(None, 'width'), may hold values from -4 to 4
- rates: float32 [2048], P('width'), may hold values from 0.001 to 0.105
- w_down: bfloat16 [2048, 2048], P(('tm', 'batch'), 'width'), may hold values from -0.125 to 0.125
- w_policy: bfloat16 [2048, 362], P('width'), may hold values from -12 to 12
- w_value: bfloat16 [2048], P('width'), may hold values from -0.125 to 0.125
Outputs:
- position_loss: float32 [8, 1024], P('batch', 'tm')
- value: float32 [8, 1024], P('batch', 'tm')
The draws below stay inside these ranges and needn't reach their ends.
All inputs are finite; a program needn't handle non-finite values.
Results may differ from the reference program's by a relative error of at most 0.0033.
Values may be sent and summed in bfloat16 or wider, within the bound.
A program may use at most 128 MiB of HBM per device.

```python
import math
import jax
import jax.numpy as jnp
from jax import lax

D = 2048
R = 2048
MOVES = 362
KERNEL = 4
GAMES = 8
TIME = 1024


def draw_w_policy(key, part):
    first = jax.random.fold_in(jax.random.fold_in(key, 17), 0)
    base = jax.random.normal(first, (D, MOVES), jnp.float32) / math.sqrt(D)
    return jnp.clip(base, -12.0, 12.0).astype(jnp.bfloat16)


def set_ends(values, rng, least, largest):
    longest = values.shape.index(max(values.shape))
    spots = []
    for shift in (0, 1):
        where = [jax.random.randint(jax.random.fold_in(rng, axis), (), 0, length) for axis, length in enumerate(values.shape)]
        where[longest] = (where[longest] + shift) % values.shape[longest]
        spots.append(tuple(where))
    return values.at[spots[0]].set(least).at[spots[1]].set(largest)


def shard_levels(rng, dims, cuts, least, top_value):
    def one(axis_at, shards_of):
        steps = jax.random.uniform(jax.random.fold_in(jax.random.fold_in(rng, 6), axis_at), (shards_of,), jnp.float32, least / len(cuts), top_value / len(cuts))
        return jnp.repeat(jnp.exp(steps), dims[axis_at] // shards_of).reshape((-1,) + (1,) * (len(dims) - axis_at - 1))

    level = one(*cuts[0])
    for cut in cuts[1:]:
        level = level * one(*cut)
    return level


def gaussian(stream_key, extent, deviation, reach, cuts=(), kind=jnp.bfloat16):
    level = shard_levels(stream_key, extent, cuts, -0.22, 0.18) if cuts else 1.0
    entries = jax.random.normal(stream_key, extent, jnp.float32) * deviation * level
    return jnp.minimum(jnp.maximum(entries, -reach), reach).astype(kind)


def setup_inputs(seed: int = 0) -> dict:
    key_list = jax.random.split(jax.random.key(seed), 12)
    moves = set_ends(jax.random.randint(key_list[0], (GAMES, TIME), 0, MOVES), jax.random.fold_in(key_list[0], 1), 0, MOVES - 1).astype(jnp.int32)
    lengths = set_ends(jax.random.randint(key_list[1], (GAMES,), 1, TIME + 1), jax.random.fold_in(key_list[1], 1), 1, TIME).astype(jnp.int32)
    outcomes = set_ends(jax.random.randint(key_list[2], (GAMES,), -1, 2), jax.random.fold_in(key_list[2], 1), -1, 1).astype(jnp.int32)
    embedded = gaussian(key_list[3], (GAMES, TIME, D), 1.0, 6.0, ((0, 4), (1, 4), (2, 2)))
    w_branches = gaussian(key_list[4], (4, D, R), D ** -0.5, 0.125, ((1, 16), (2, 2)))
    conv_w = gaussian(key_list[5], (KERNEL, R), 0.5, 3.0, ((1, 2),), jnp.float32)
    gate_bias = gaussian(key_list[6], (2, R), 1.0, 4.0, ((1, 2),), jnp.float32)
    rates = jnp.clip(jnp.exp(math.log(0.105) - 4.65396 * jax.random.uniform(key_list[7], (R,), jnp.float32) ** shard_levels(key_list[7], (R,), ((0, 2),), -0.2, 0.2)), 0.001, 0.105)
    w_down = gaussian(key_list[8], (D, R), R ** -0.5, 0.125, ((0, 16), (1, 2)))
    w_policy = draw_w_policy(jax.random.fold_in(key_list[11], 71), 0)
    w_value = gaussian(key_list[10], (D,), D ** -0.5, 0.125, ((0, 2),))
    return {"moves": moves, "lengths": lengths, "outcomes": outcomes, "embedded": embedded, "w_branches": w_branches, "conv_w": conv_w, "gate_bias": gate_bias, "rates": rates, "w_down": w_down, "w_policy": w_policy, "w_value": w_value}


def link(early, late):
    return (early[0] + late[0], jnp.exp(late[0]) * early[1] + late[1])

def reference(moves, lengths, outcomes, embedded, w_branches, conv_w, gate_bias, rates, w_down, w_policy, w_value):

    def one_game(packed):
        feats, played, length, result = packed
        proj = [jnp.dot(feats, w_branches[k], preferred_element_type=jnp.float32) for k in range(4)]
        gated = jax.nn.gelu(proj[0])
        padded = jnp.concatenate([jnp.zeros((KERNEL - 1, R), jnp.float32), proj[1]], 0)
        conv = jnp.zeros((TIME, R), jnp.float32)
        for k in range(KERNEL):
            conv = conv + conv_w[k] * padded[KERNEL - 1 - k:KERNEL - 1 - k + TIME]
        recur = jax.nn.sigmoid(proj[2] + gate_bias[0])
        inflow = jax.nn.sigmoid(proj[3] + gate_bias[1])
        log_a = -8.0 * recur * rates
        decay = jnp.exp(log_a)
        drive = jnp.sqrt(1.0 - decay * decay) * inflow * conv
        summed, hidden = lax.associative_scan(link, (log_a, drive), axis=0)
        mixed = (hidden * gated).astype(jnp.bfloat16)
        down = lax.dot_general(mixed, w_down, (((1,), (1,)), ((), ())), preferred_element_type=jnp.float32)
        resid = (feats.astype(jnp.float32) + down).astype(jnp.bfloat16)
        wide = resid.astype(jnp.float32)
        sumsq = lax.optimization_barrier(jnp.sum(wide * wide, -1))
        norm = lax.rsqrt(sumsq / D + 1e-06)
        logits = jnp.dot(resid, w_policy, preferred_element_type=jnp.float32) * norm[:, None]
        value = jnp.tanh(jnp.dot(resid, w_value, preferred_element_type=jnp.float32) * norm)
        top = lax.optimization_barrier(jnp.max(logits, -1, keepdims=True))
        lse = top[:, 0] + jnp.log(lax.optimization_barrier(jnp.sum(jnp.exp(logits - top), -1)))
        column = lax.broadcasted_iota(jnp.int32, (TIME, MOVES), 1)
        picked = lax.optimization_barrier(jnp.sum(jnp.where(column == played[:, None], logits, 0.0), -1))
        target = result.astype(jnp.float32)
        where_live = jnp.arange(TIME, dtype=jnp.int32) < length
        loss = jnp.where(where_live, lse - picked + (value - target) ** 2, 0.0)
        return (loss, value)
    return lax.map(one_game, (embedded, moves, lengths, outcomes))
```

```python
import functools

import jax
import jax.numpy as jnp
from jax import lax
from jax.experimental import pallas as pl
from jax.experimental.pallas import tpu as pltpu
from jax.sharding import PartitionSpec as P

KERNEL = 4
SUB = 8


def swap(value, axis):
    n = lax.axis_size(axis)
    return lax.ppermute(value, axis, [(i, n - 1 - i) for i in range(n)])


def from_behind(value, axis):
    n = lax.axis_size(axis)
    return lax.ppermute(value, axis, [(i, i + 1) for i in range(n - 1)])


def interleave(x):
    games, steps = x.shape[:2]
    return jnp.swapaxes(x.reshape(games, SUB, steps // SUB, *x.shape[2:]), 1, 2).reshape(x.shape)


def restore(x):
    games, steps = x.shape[:2]
    return jnp.swapaxes(x.reshape(games, steps // SUB, SUB, *x.shape[2:]), 1, 2).reshape(x.shape)


def both(own, other, axis, dim):
    first = lax.axis_index(axis) == 0
    return jnp.concatenate([jnp.where(first, own, other), jnp.where(first, other, own)], dim)


def scan_kernel(
    proj, halo, conv_w, bias, rates, hg, pg, ends, h_s, p_s, g_s, carry_s
):
    steps, cols = proj.shape[1], proj.shape[2]
    seg = steps // SUB
    w = [conv_w[k : k + 1, :] for k in range(KERNEL)]
    b0, b1 = bias[0:1, :], bias[1:2, :]
    scale = -8.0 * rates[0:1, :]
    row = lax.broadcasted_iota(jnp.int32, (SUB, cols), 0)

    def rows(k, t):
        return proj[k, pl.ds(pl.multiple_of(t * SUB, SUB), SUB), :]

    def before(j):
        rolled = pltpu.roll(rows(1, seg - j), 1, 0)
        return jnp.where(row == 0, halo[0, KERNEL - 1 - j : KERNEL - j, :], rolled)

    def step(t, state):
        h, p, x1, x2, x3 = state
        x0 = rows(1, t)
        conv = w[0] * x0 + w[1] * x1 + w[2] * x2 + w[3] * x3
        recur = jax.nn.sigmoid(rows(2, t) + b0)
        inflow = jax.nn.sigmoid(rows(3, t) + b1)
        a = jnp.exp(recur * scale)
        h = a * h + jnp.sqrt(1.0 - a * a) * inflow * conv
        p = a * p
        h_s[t] = h
        p_s[t] = p
        g_s[t] = jax.nn.gelu(rows(0, t))
        return h, p, x0, x1, x2

    zero = jnp.zeros((SUB, cols), jnp.float32)
    h, p, _, _, _ = lax.fori_loop(
        0, seg, step, (zero, zero + 1.0, before(1), before(2), before(3)), unroll=4
    )
    run, dec = jnp.zeros((1, cols), jnp.float32), jnp.ones((1, cols), jnp.float32)
    for s in range(SUB):
        carry_s[0, s : s + 1, :] = run
        carry_s[1, s : s + 1, :] = dec
        run = p[s : s + 1] * run + h[s : s + 1]
        dec = p[s : s + 1] * dec
    ends[0, 0:1, :] = run
    ends[0, 1:2, :] = dec
    run, dec = carry_s[0], carry_s[1]

    def finish(t, _):
        g, p = g_s[t], p_s[t]
        hg[pl.ds(pl.multiple_of(t * SUB, SUB), SUB), :] = (h_s[t] + p * run) * g
        pg[pl.ds(pl.multiple_of(t * SUB, SUB), SUB), :] = p * dec * g
        return 0

    lax.fori_loop(0, seg, finish, 0, unroll=4)


def block_scan(proj, halo, conv_w, gate_bias, rates, games):
    _, count, chans = proj.shape
    steps = count // games
    cols = min(512, chans)
    return pl.pallas_call(
        scan_kernel,
        grid=(games, chans // cols),
        in_specs=[
            pl.BlockSpec((4, steps, cols), lambda g, c: (0, g, c)),
            pl.BlockSpec((1, KERNEL - 1, cols), lambda g, c: (g, 0, c)),
            pl.BlockSpec((KERNEL, cols), lambda g, c: (0, c)),
            pl.BlockSpec((2, cols), lambda g, c: (0, c)),
            pl.BlockSpec((1, cols), lambda g, c: (0, c)),
        ],
        out_specs=[
            pl.BlockSpec((steps, cols), lambda g, c: (g, c)),
            pl.BlockSpec((steps, cols), lambda g, c: (g, c)),
            pl.BlockSpec((1, 2, cols), lambda g, c: (g, 0, c)),
        ],
        out_shape=[
            jax.ShapeDtypeStruct((count, chans), jnp.float32),
            jax.ShapeDtypeStruct((count, chans), jnp.float32),
            jax.ShapeDtypeStruct((games, 2, chans), jnp.float32),
        ],
        scratch_shapes=[pltpu.VMEM((steps // SUB, SUB, cols), jnp.float32)] * 3
        + [pltpu.VMEM((2, SUB, cols), jnp.float32)],
        cost_estimate=pl.CostEstimate(
            flops=60 * count * chans, bytes_accessed=24 * count * chans, transcendentals=8 * count * chans
        ),
    )(proj, halo, conv_w, gate_bias, rates.reshape(1, chans))


def shards(
    moves,
    lengths,
    outcomes,
    embedded,
    w_branches,
    conv_w,
    gate_bias,
    rates,
    w_down,
    w_policy,
    w_value,
):
    games, block_len, half = embedded.shape
    count = games * block_len
    chans = w_branches.shape[2]
    n_width = lax.axis_size("width")
    me = lax.axis_index("width")
    own_rows = count // n_width

    flat = interleave(embedded).reshape(count, half)
    features = both(flat, swap(flat, "width"), "width", 1)
    heads = jnp.concatenate([w_policy, w_value[:, None]], 1)
    heads = both(heads, swap(heads, "width"), "width", 0)
    depth = features.shape[1]
    tail = features.reshape(games, block_len // SUB, SUB, depth)[:, 1 - KERNEL :, SUB - 1, :]
    tail = from_behind(tail, "tm").reshape(games * (KERNEL - 1), depth)

    w_full = lax.all_gather(w_branches, ("tm", "batch"), axis=1, tiled=True)
    proj = jnp.einsum("td,kdn->ktn", features, w_full, preferred_element_type=jnp.float32)
    halo = jnp.dot(tail, w_full[1], preferred_element_type=jnp.float32)
    hg, pg, ends = block_scan(
        proj, halo.reshape(games, KERNEL - 1, chans), conv_w, gate_bias, rates, games
    )
    w_out = lax.all_gather(w_down, ("tm", "batch"), axis=0, tiled=True)
    ends_all = lax.all_gather(ends, "tm", axis=0)
    state = jnp.zeros((games, chans), jnp.float32)
    here = lax.axis_index("tm")
    for j in range(lax.axis_size("tm") - 1):
        state = jnp.where(j < here, ends_all[j, :, 1] * state + ends_all[j, :, 0], state)
    mixed = hg.reshape(games, block_len, chans) + pg.reshape(games, block_len, chans) * state[:, None]
    mixed = mixed.astype(jnp.bfloat16).reshape(count, chans)

    def down_of(owner):
        return lax.dot_general(
            lax.dynamic_slice_in_dim(mixed, owner * own_rows, own_rows, 0),
            w_out,
            (((1,), (1,)), ((), ())),
            preferred_element_type=jnp.float32,
        )

    sent = swap(down_of(n_width - 1 - me).astype(jnp.bfloat16), "width")
    down = down_of(me) + sent.astype(jnp.float32)

    def mine(x):
        return lax.dynamic_slice_in_dim(x, me * own_rows, own_rows, 0)

    resid = (mine(features).astype(jnp.float32) + down).astype(jnp.bfloat16)
    wide = resid.astype(jnp.float32)
    sumsq = jnp.sum(wide * wide, -1)
    scores = jnp.dot(resid, heads, preferred_element_type=jnp.float32)
    norm = lax.rsqrt(sumsq / depth + 1e-06)
    scores = scores * norm[:, None]
    logits = scores[:, :-1]
    value = jnp.tanh(scores[:, -1])
    top = jnp.max(logits, -1, keepdims=True)
    lse = top[:, 0] + jnp.log(jnp.sum(jnp.exp(logits - top), -1))
    column = lax.broadcasted_iota(jnp.int32, logits.shape, 1)
    picked = jnp.sum(jnp.where(column == mine(interleave(moves).reshape(count, 1)), logits, 0.0), -1)
    target = jnp.broadcast_to(outcomes.astype(jnp.float32)[:, None], (games, block_len))
    position = here * block_len + lax.broadcasted_iota(jnp.int32, (games, block_len), 1)
    live = interleave(position < lengths[:, None]).reshape(count)
    loss = jnp.where(mine(live), lse - picked + (value - mine(target.reshape(count))) ** 2, 0.0)
    result = jnp.stack([loss, value])
    result = both(result, swap(result, "width"), "width", 1)
    result = result.reshape(2, games, block_len)
    return (restore(result[0]), restore(result[1]))


def solution(mesh):
    in_specs = (
        P("batch", "tm"),
        P("batch"),
        P("batch"),
        P("batch", "tm", "width"),
        P(None, ("tm", "batch"), "width"),
        P(None, "width"),
        P(None, "width"),
        P("width"),
        P(("tm", "batch"), "width"),
        P("width", None),
        P("width"),
    )
    out_specs = (P("batch", "tm"), P("batch", "tm"))
    return jax.shard_map(shards, mesh=mesh, in_specs=in_specs, out_specs=out_specs, check_vma=False)
```

```python
import jax
import jax.numpy as jnp
from jax import lax
from jax.experimental import pallas as pl
from jax.experimental.pallas import tpu as pltpu
from jax.sharding import PartitionSpec as P

KERNEL = 4
SUB = 8
MESH = pl.DeviceIdType.MESH
STREAMS = tuple(range(6))


def swap(value, axis):
    n = lax.axis_size(axis)
    return lax.ppermute(value, axis, [(i, n - 1 - i) for i in range(n)])


def interleave(x):
    games, steps = x.shape[:2]
    return jnp.swapaxes(x.reshape(games, SUB, steps // SUB, *x.shape[2:]), 1, 2).reshape(x.shape)


def restore(x):
    games, steps = x.shape[:2]
    return jnp.swapaxes(x.reshape(games, steps // SUB, SUB, *x.shape[2:]), 1, 2).reshape(x.shape)


def both(own, other, axis, dim):
    first = lax.axis_index(axis) == 0
    return jnp.concatenate([jnp.where(first, own, other), jnp.where(first, other, own)], dim)


def core_kernel(
    emb, wb, wd, tail, conv_w, bias, rates,
    hg, pg, ends, wd_all, feat,
    w_all, acc, tails, halo, carry_s,
    loc, feat_s, feat_r, tail_s, tail_r, ring_s, ring_r, peer_s, peer_r,
):
    z, b, y = lax.axis_index("tm"), lax.axis_index("batch"), lax.axis_index("width")
    zn, bn, yn = lax.axis_size("tm"), lax.axis_size("batch"), lax.axis_size("width")
    x, core = b // 2, b % 2
    n = zn * (bn // 2)
    rows, chans = wd.shape
    count, half = emb.shape
    games = ends.shape[0]
    width_cut = chans // 2

    def spot(r):
        cx = r // zn
        cz = r % zn
        return cz + (cx % 2) * (zn - 1 - 2 * cz), cx

    r = x * zn + z + (x % 2) * (zn - 1 - 2 * z)

    def at(place, c=core, w=y):
        return {"tm": place[0], "batch": place[1] * 2 + c, "width": w}

    ahead, behind = at(spot((r + 1) % n)), at(spot((r + n - 1) % n))
    peer = at((z, x), 1 - core)
    partner = at((z, x), core, yn - 1 - y)
    later, earlier = ((z + 1) % zn, x), ((z + zn - 1) % zn, x)
    tail_to = [at(later), at(later, core, yn - 1 - y)]
    greet = [ahead, behind, peer, partner] + tail_to + [at(earlier), at(earlier, core, yn - 1 - y)]

    def first_row(chip):
        cz, cx = spot(chip)
        return (cz * bn + cx * 2) * rows

    own = first_row(r) + core * rows
    own = pl.multiple_of(own, rows)
    local = [
        pltpu.make_async_copy(wb, w_all.at[:, pl.ds(own, rows), :], loc.at[0]),
        pltpu.make_async_copy(wd, wd_all.at[pl.ds(own, rows), :], loc.at[1]),
        pltpu.make_async_copy(emb, feat.at[y], loc.at[2]),
        pltpu.make_async_copy(tail, tails.at[2], loc.at[3]),
    ]
    for copy in local:
        copy.start()
    barrier = pltpu.get_barrier_semaphore()
    for device in greet:
        pl.semaphore_signal(barrier, inc=1, device_id=device, device_id_type=MESH)
    pl.semaphore_wait(barrier, len(greet))
    for copy in local:
        copy.wait()

    def remote(src, dst, send, recv, device):
        return pltpu.make_async_remote_copy(
            src_ref=src, dst_ref=dst, send_sem=send, recv_sem=recv, device_id=device, device_id_type=MESH
        )

    def forward(s):
        return s in (0, 1, 4)

    def chip_of(s, t):
        return (r + n - t) % n if forward(s) else (r + t) % n

    def piece(s, chip, c):
        at_row = pl.ds(pl.multiple_of(first_row(chip) + c * rows, rows), rows)
        if s < 4:
            return w_all.at[s, at_row, :]
        return wd_all.at[at_row, pl.ds((s - 4) * width_cut, width_cut)]

    def hop(s, t):
        ref = piece(s, chip_of(s, t - 1), core)
        return remote(ref, ref, ring_s.at[s, t], ring_r.at[s, t], ahead if forward(s) else behind)

    def landed(s, t):
        ref = piece(s, chip_of(s, t), core)
        return remote(ref, ref, ring_s.at[s, t], ring_r.at[s, t], ahead if forward(s) else behind)

    def share(s, t):
        ref = piece(s, chip_of(s, t), core)
        return remote(ref, ref, peer_s.at[s, t], peer_r.at[s, t], peer)

    def shared(s, t):
        ref = piece(s, chip_of(s, t), 1 - core)
        return remote(ref, ref, peer_s.at[s, t], peer_r.at[s, t], peer)

    for s in STREAMS:
        hop(s, 1).start()
    swap_feat = remote(feat.at[y], feat.at[y], feat_s, feat_r, partner)
    swap_feat.start()
    tail_out = [
        remote(tails.at[2], tails.at[y], tail_s.at[i], tail_r.at[i], tail_to[i]) for i in range(2)
    ]
    for copy in tail_out:
        copy.start()
    for s in STREAMS:
        share(s, 0).start()
    acc[...] = jnp.zeros_like(acc)
    ref = feat.at[yn - 1 - y]
    remote(ref, ref, feat_s, feat_r, partner).wait_recv()

    tile = min(512, chans)
    eager = (2 * rows) % 128 == 0

    def product(s, start, depth):
        owner, col = start // half, pl.multiple_of(start % half, depth)
        left = feat[owner, :, pl.ds(col, depth)]

        @pl.loop(0, chans // tile)
        def _(j):
            cut = pl.ds(pl.multiple_of(j * tile, tile), tile)
            acc[s, :, cut] += jnp.dot(
                left,
                w_all[s, pl.ds(pl.multiple_of(start, depth), depth), cut],
                preferred_element_type=jnp.float32,
            )

    def compute(t):
        for s in STREAMS:
            shared(s, t).wait_recv()
            if s < 4 and eager:
                product(s, first_row(chip_of(s, t)), 2 * rows)

    @pl.loop(1, n)
    def _(t):
        for s in STREAMS:
            landed(s, t).wait_recv()

            @pl.when(t < n - 1)
            def _():
                hop(s, t + 1).start()

            share(s, t).start()
        compute(t - 1)

    compute(n - 1)
    if not eager:
        depth = min(256, half)

        @pl.loop(0, yn * half // depth)
        def _(i):
            for s in range(4):
                product(s, i * depth, depth)

    for i in range(2):
        ref = tails.at[y if i == 0 else yn - 1 - y]
        remote(ref, ref, tail_s.at[i], tail_r.at[i], tail_to[i]).wait_recv()
    cols = min(512, chans)
    blocks = chans // cols

    @pl.loop(0, blocks)
    def _(j):
        cut = pl.ds(pl.multiple_of(j * cols, cols), cols)
        edge = jnp.zeros((tails.shape[1], cols), jnp.float32)
        for owner in range(yn):
            edge += jnp.dot(
                tails[owner],
                w_all[1, owner * half : (owner + 1) * half, cut],
                preferred_element_type=jnp.float32,
            )
        halo[:, cut] = jnp.where(z > 0, edge, 0.0)

    steps = count // games
    seg = steps // SUB

    @pl.loop(0, games * blocks)
    def _(u):
        g, j = u // blocks, u % blocks
        cut = pl.ds(pl.multiple_of(j * cols, cols), cols)
        scan_block(
            acc, halo[pl.ds(pl.multiple_of(g * SUB, SUB), SUB), cut], conv_w[:, cut], bias[:, cut], rates[:, cut],
            hg, pg, ends, carry_s, g, cut, cols, seg,
        )

    for s in STREAMS:

        @pl.loop(1, n)
        def _(t):
            hop(s, t).wait_send()

        @pl.loop(0, n)
        def _(t):
            share(s, t).wait_send()

    swap_feat.wait_send()
    for copy in tail_out:
        copy.wait_send()


def scan_block(acc, halo, conv_w, bias, rates, hg, pg, ends, carry_s, g, cut, cols, seg):
    w = [conv_w[k : k + 1, :] for k in range(KERNEL)]
    b0, b1 = bias[0:1, :], bias[1:2, :]
    scale = -8.0 * rates
    row = lax.broadcasted_iota(jnp.int32, (SUB, cols), 0)

    def at(t):
        return pl.ds(pl.multiple_of((g * seg + t) * SUB, SUB), SUB)

    def before(j):
        rolled = pltpu.roll(acc[1, at(seg - j), cut], 1, 0)
        return jnp.where(row == 0, halo[KERNEL - 1 - j : KERNEL - j, :], rolled)

    def step(t, state):
        h, p, x1, x2, x3 = state
        here = at(t)
        x0 = acc[1, here, cut]
        conv = w[0] * x0 + w[1] * x1 + w[2] * x2 + w[3] * x3
        recur = jax.nn.sigmoid(acc[2, here, cut] + b0)
        inflow = jax.nn.sigmoid(acc[3, here, cut] + b1)
        a = jnp.exp(recur * scale)
        h = a * h + jnp.sqrt(1.0 - a * a) * inflow * conv
        p = a * p
        acc[0, here, cut] = jax.nn.gelu(acc[0, here, cut])
        acc[2, here, cut] = h
        acc[3, here, cut] = p
        return h, p, x0, x1, x2

    zero = jnp.zeros((SUB, cols), jnp.float32)
    h, p, _, _, _ = lax.fori_loop(
        0, seg, step, (zero, zero + 1.0, before(1), before(2), before(3)), unroll=4
    )
    run, dec = jnp.zeros((1, cols), jnp.float32), jnp.ones((1, cols), jnp.float32)
    for s in range(SUB):
        carry_s[0, s : s + 1, :] = run
        carry_s[1, s : s + 1, :] = dec
        run = p[s : s + 1] * run + h[s : s + 1]
        dec = p[s : s + 1] * dec
    ends[g, 0:1, cut] = run
    ends[g, 1:2, cut] = dec
    run, dec = carry_s[0], carry_s[1]

    def finish(t, _):
        here = at(t)
        gate, p = acc[0, here, cut], acc[3, here, cut]
        hg[here, cut] = (acc[2, here, cut] + p * run) * gate
        pg[here, cut] = p * dec * gate
        return 0

    lax.fori_loop(0, seg, finish, 0, unroll=4)


def core_block(emb, wb, wd, tail, conv_w, bias, rates, games):
    count, half = emb.shape
    rows, chans = wd.shape
    yn = lax.axis_size("width")
    n = lax.axis_size("tm") * (lax.axis_size("batch") // 2)
    depth = yn * half
    vmem = pl.BlockSpec(memory_space=pltpu.VMEM)
    hbm = pl.BlockSpec(memory_space=pl.ANY)
    dma = pltpu.SemaphoreType.DMA
    streams = len(STREAMS)
    return pl.pallas_call(
        core_kernel,
        in_specs=[hbm] * 4 + [vmem] * 3,
        out_specs=[vmem] * 5,
        out_shape=[
            jax.ShapeDtypeStruct((count, chans), jnp.float32),
            jax.ShapeDtypeStruct((count, chans), jnp.float32),
            jax.ShapeDtypeStruct((games, 2, chans), jnp.float32),
            jax.ShapeDtypeStruct((depth, chans), jnp.bfloat16),
            jax.ShapeDtypeStruct((yn, count, half), jnp.bfloat16),
        ],
        scratch_shapes=[
            pltpu.VMEM((4, depth, chans), jnp.bfloat16),
            pltpu.VMEM((4, count, chans), jnp.float32),
            pltpu.VMEM((3, games * SUB, half), jnp.bfloat16),
            pltpu.VMEM((games * SUB, chans), jnp.float32),
            pltpu.VMEM((2, SUB, min(512, chans)), jnp.float32),
            dma((4,)), dma, dma, dma((2,)), dma((2,)),
            dma((streams, n)), dma((streams, n)), dma((streams, n)), dma((streams, n)),
        ],
        compiler_params=pltpu.CompilerParams(
            collective_id=0, has_side_effects=True, vmem_limit_bytes=56 * 1024 * 1024
        ),
        cost_estimate=pl.CostEstimate(
            flops=8 * count * chans * depth, bytes_accessed=200_000_000, transcendentals=8 * count * chans
        ),
    )(emb, wb, wd, tail, conv_w, bias, rates.reshape(1, chans))


def shards(
    moves,
    lengths,
    outcomes,
    embedded,
    w_branches,
    conv_w,
    gate_bias,
    rates,
    w_down,
    w_policy,
    w_value,
):
    games, block_len, half = embedded.shape
    count = games * block_len
    chans = w_branches.shape[2]
    n_width = lax.axis_size("width")
    me = lax.axis_index("width")
    own_rows = count // n_width

    flat = interleave(embedded).reshape(count, half)
    heads = jnp.concatenate([w_policy, w_value[:, None]], 1)
    heads = both(heads, swap(heads, "width"), "width", 0)
    depth = n_width * half
    tail = flat.reshape(games, block_len // SUB, SUB, half)[:, 1 - KERNEL :, SUB - 1, :]
    tail = jnp.pad(tail, ((0, 0), (0, SUB + 1 - KERNEL), (0, 0))).reshape(games * SUB, half)
    hg, pg, ends, w_out, feat = core_block(
        flat, w_branches, w_down, tail, conv_w, gate_bias, rates, games
    )
    ends_all = lax.all_gather(ends, "tm", axis=0)
    state = jnp.zeros((games, chans), jnp.float32)
    here = lax.axis_index("tm")
    for j in range(lax.axis_size("tm") - 1):
        state = jnp.where(j < here, ends_all[j, :, 1] * state + ends_all[j, :, 0], state)
    mixed = hg.reshape(games, block_len, chans) + pg.reshape(games, block_len, chans) * state[:, None]
    mixed = mixed.astype(jnp.bfloat16).reshape(count, chans)

    def down_of(owner):
        return lax.dot_general(
            lax.dynamic_slice_in_dim(mixed, owner * own_rows, own_rows, 0),
            w_out,
            (((1,), (1,)), ((), ())),
            preferred_element_type=jnp.float32,
        )

    sent = swap(down_of(n_width - 1 - me).astype(jnp.bfloat16), "width")
    down = down_of(me) + sent.astype(jnp.float32)

    def mine(x):
        return lax.dynamic_slice_in_dim(x, me * own_rows, own_rows, 0)

    features = jnp.concatenate([mine(feat[i]) for i in range(n_width)], 1)
    resid = (features.astype(jnp.float32) + down).astype(jnp.bfloat16)
    wide = resid.astype(jnp.float32)
    sumsq = jnp.sum(wide * wide, -1)
    scores = jnp.dot(resid, heads, preferred_element_type=jnp.float32)
    norm = lax.rsqrt(sumsq / depth + 1e-06)
    scores = scores * norm[:, None]
    logits = scores[:, :-1]
    value = jnp.tanh(scores[:, -1])
    top = jnp.max(logits, -1, keepdims=True)
    lse = top[:, 0] + jnp.log(jnp.sum(jnp.exp(logits - top), -1))
    column = lax.broadcasted_iota(jnp.int32, logits.shape, 1)
    picked = jnp.sum(jnp.where(column == mine(interleave(moves).reshape(count, 1)), logits, 0.0), -1)
    target = jnp.broadcast_to(outcomes.astype(jnp.float32)[:, None], (games, block_len))
    position = here * block_len + lax.broadcasted_iota(jnp.int32, (games, block_len), 1)
    live = interleave(position < lengths[:, None]).reshape(count)
    loss = jnp.where(mine(live), lse - picked + (value - mine(target.reshape(count))) ** 2, 0.0)
    result = jnp.stack([loss, value])
    result = both(result, swap(result, "width"), "width", 1)
    result = result.reshape(2, games, block_len)
    return (restore(result[0]), restore(result[1]))


def solution(mesh):
    in_specs = (
        P("batch", "tm"),
        P("batch"),
        P("batch"),
        P("batch", "tm", "width"),
        P(None, ("tm", "batch"), "width"),
        P(None, "width"),
        P(None, "width"),
        P("width"),
        P(("tm", "batch"), "width"),
        P("width", None),
        P("width"),
    )
    out_specs = (P("batch", "tm"), P("batch", "tm"))
    return jax.shard_map(shards, mesh=mesh, in_specs=in_specs, out_specs=out_specs, check_vma=False)
```

```python
import jax
import jax.numpy as jnp
from jax import lax
from jax.experimental import pallas as pl
from jax.experimental.pallas import tpu as pltpu
from jax.sharding import PartitionSpec as P

KERNEL = 4
SUB = 8
MESH = pl.DeviceIdType.MESH
STREAMS = tuple(range(6))


def swap(value, axis):
    n = lax.axis_size(axis)
    return lax.ppermute(value, axis, [(i, n - 1 - i) for i in range(n)])


def interleave(x):
    games, steps = x.shape[:2]
    return jnp.swapaxes(x.reshape(games, SUB, steps // SUB, *x.shape[2:]), 1, 2).reshape(x.shape)


def restore(x):
    games, steps = x.shape[:2]
    return jnp.swapaxes(x.reshape(games, steps // SUB, SUB, *x.shape[2:]), 1, 2).reshape(x.shape)


def both(own, other, axis, dim):
    first = lax.axis_index(axis) == 0
    return jnp.concatenate([jnp.where(first, own, other), jnp.where(first, other, own)], dim)


def core_kernel(
    emb, wb, wd, tail, conv_w, bias, rates,
    resid,
    w_all, acc, tails, halo, carry_s, wd_all, feat, ends, state, mixed, out_buf, in_buf, kept,
    loc, feat_s, feat_r, tail_s, tail_r, ring_s, ring_r, peer_s, peer_r, ends_s, ends_r, out_s, out_r,
):
    z, b, y = lax.axis_index("tm"), lax.axis_index("batch"), lax.axis_index("width")
    zn, bn, yn = lax.axis_size("tm"), lax.axis_size("batch"), lax.axis_size("width")
    x, core = b // 2, b % 2
    n = zn * (bn // 2)
    rows, chans = wd.shape
    count, half = emb.shape
    games = ends.shape[1]
    width_cut = chans // 2

    def spot(r):
        cx = r // zn
        cz = r % zn
        return cz + (cx % 2) * (zn - 1 - 2 * cz), cx

    r = x * zn + z + (x % 2) * (zn - 1 - 2 * z)

    def at(place, c=core, w=y):
        return {"tm": place[0], "batch": place[1] * 2 + c, "width": w}

    ahead, behind = at(spot((r + 1) % n)), at(spot((r + n - 1) % n))
    peer = at((z, x), 1 - core)
    partner = at((z, x), core, yn - 1 - y)
    later, earlier = ((z + 1) % zn, x), ((z + zn - 1) % zn, x)
    tail_to = [at(later), at(later, core, yn - 1 - y)]
    greet = [ahead, behind, peer, partner] + tail_to + [at(earlier), at(earlier, core, yn - 1 - y)]
    greet += [at(((z + d) % zn, x)) for d in range(2, zn - 1)]

    def first_row(chip):
        cz, cx = spot(chip)
        return (cz * bn + cx * 2) * rows

    own = first_row(r) + core * rows
    own = pl.multiple_of(own, rows)
    local = [
        pltpu.make_async_copy(wb, w_all.at[:, pl.ds(own, rows), :], loc.at[0]),
        pltpu.make_async_copy(wd, wd_all.at[pl.ds(own, rows), :], loc.at[1]),
        pltpu.make_async_copy(emb, feat.at[y], loc.at[2]),
        pltpu.make_async_copy(tail, tails.at[2], loc.at[3]),
    ]
    for copy in local:
        copy.start()
    barrier = pltpu.get_barrier_semaphore()
    for device in greet:
        pl.semaphore_signal(barrier, inc=1, device_id=device, device_id_type=MESH)
    pl.semaphore_wait(barrier, len(greet))
    for copy in local:
        copy.wait()

    def remote(src, dst, send, recv, device):
        return pltpu.make_async_remote_copy(
            src_ref=src, dst_ref=dst, send_sem=send, recv_sem=recv, device_id=device, device_id_type=MESH
        )

    def forward(s):
        return s in (0, 1, 4)

    def chip_of(s, t):
        return (r + n - t) % n if forward(s) else (r + t) % n

    def piece(s, chip, c):
        at_row = pl.ds(pl.multiple_of(first_row(chip) + c * rows, rows), rows)
        if s < 4:
            return w_all.at[s, at_row, :]
        return wd_all.at[at_row, pl.ds((s - 4) * width_cut, width_cut)]

    def hop(s, t):
        ref = piece(s, chip_of(s, t - 1), core)
        return remote(ref, ref, ring_s.at[s, t], ring_r.at[s, t], ahead if forward(s) else behind)

    def landed(s, t):
        ref = piece(s, chip_of(s, t), core)
        return remote(ref, ref, ring_s.at[s, t], ring_r.at[s, t], ahead if forward(s) else behind)

    def share(s, t):
        ref = piece(s, chip_of(s, t), core)
        return remote(ref, ref, peer_s.at[s, t], peer_r.at[s, t], peer)

    def shared(s, t):
        ref = piece(s, chip_of(s, t), 1 - core)
        return remote(ref, ref, peer_s.at[s, t], peer_r.at[s, t], peer)

    for s in STREAMS:
        hop(s, 1).start()
    swap_feat = remote(feat.at[y], feat.at[y], feat_s, feat_r, partner)
    swap_feat.start()
    tail_out = [
        remote(tails.at[2], tails.at[y], tail_s.at[i], tail_r.at[i], tail_to[i]) for i in range(2)
    ]
    for copy in tail_out:
        copy.start()
    for s in STREAMS:
        share(s, 0).start()
    acc[...] = jnp.zeros_like(acc)
    ref = feat.at[yn - 1 - y]
    remote(ref, ref, feat_s, feat_r, partner).wait_recv()

    tile = min(512, chans)
    eager = (2 * rows) % 128 == 0

    def product(s, start, depth):
        owner, col = start // half, pl.multiple_of(start % half, depth)
        left = feat[owner, :, pl.ds(col, depth)]

        @pl.loop(0, chans // tile)
        def _(j):
            cut = pl.ds(pl.multiple_of(j * tile, tile), tile)
            acc[s, :, cut] += jnp.dot(
                left,
                w_all[s, pl.ds(pl.multiple_of(start, depth), depth), cut],
                preferred_element_type=jnp.float32,
            )

    def compute(t):
        for s in STREAMS:
            shared(s, t).wait_recv()
            if s < 4 and eager:
                product(s, first_row(chip_of(s, t)), 2 * rows)

    @pl.loop(1, n)
    def _(t):
        for s in STREAMS:
            landed(s, t).wait_recv()

            @pl.when(t < n - 1)
            def _():
                hop(s, t + 1).start()

            share(s, t).start()
        compute(t - 1)

    compute(n - 1)
    if not eager:
        depth = min(256, half)

        @pl.loop(0, yn * half // depth)
        def _(i):
            for s in range(4):
                product(s, i * depth, depth)

    for i in range(2):
        ref = tails.at[y if i == 0 else yn - 1 - y]
        remote(ref, ref, tail_s.at[i], tail_r.at[i], tail_to[i]).wait_recv()
    cols = min(512, chans)
    blocks = chans // cols

    @pl.loop(0, blocks)
    def _(j):
        cut = pl.ds(pl.multiple_of(j * cols, cols), cols)
        edge = jnp.zeros((tails.shape[1], cols), jnp.float32)
        for owner in range(yn):
            edge += jnp.dot(
                tails[owner],
                w_all[1, owner * half : (owner + 1) * half, cut],
                preferred_element_type=jnp.float32,
            )
        halo[:, cut] = jnp.where(z > 0, edge, 0.0)

    steps = count // games
    seg = steps // SUB

    @pl.loop(0, games * blocks)
    def _(u):
        g, j = u // blocks, u % blocks
        cut = pl.ds(pl.multiple_of(j * cols, cols), cols)
        scan_block(
            acc, halo[pl.ds(pl.multiple_of(g * SUB, SUB), SUB), cut], conv_w[:, cut], bias[:, cut], rates[:, cut],
            ends, carry_s, z, g, cut, cols, seg,
        )

    def relay(d, source):
        ref = ends.at[source]
        return remote(ref, ref, ends_s.at[d], ends_r.at[d], at(((z + d) % zn, x)))

    for d in range(1, zn):
        relay(d, z).start()
    for d in range(1, zn):
        relay(d, (z + zn - d) % zn).wait_recv()
    for g in range(games):
        run = jnp.zeros((1, chans), jnp.float32)
        for j in range(zn - 1):
            run = jnp.where(j < z, ends[j, g, 1:2, :] * run + ends[j, g, 0:1, :], run)
        state[g : g + 1, :] = run
    for g in range(games):
        run = state[g : g + 1, :]

        @pl.loop(0, steps // 16)
        def _(i):
            here = pl.ds(pl.multiple_of(g * steps + i * 16, 16), 16)
            mixed[here, :] = (acc[2, here, :] + acc[3, here, :] * run).astype(jnp.bfloat16)

    parts, own_rows, part = out_buf.shape
    mine = pl.ds(pl.multiple_of(y * own_rows, own_rows), own_rows)
    theirs = pl.ds(pl.multiple_of((yn - 1 - y) * own_rows, own_rows), own_rows)

    def down(which, j):
        return lax.dot_general(
            mixed[which, :],
            wd_all[j * part : (j + 1) * part, :],
            (((1,), (1,)), ((), ())),
            preferred_element_type=jnp.float32,
        )

    def exchange(j):
        return remote(out_buf.at[j], in_buf.at[j], out_s.at[j], out_r.at[j], partner)

    for j in range(parts):
        out_buf[j] = down(theirs, j).astype(jnp.bfloat16)
        if j:
            exchange(j - 1).start()
    kept[0] = down(mine, 0)
    exchange(parts - 1).start()
    for j in range(1, parts):
        kept[j] = down(mine, j)
    for j in range(parts):
        exchange(j).wait_recv()
        first = j * part
        base = feat[first // half, mine, first % half : first % half + part].astype(jnp.float32)
        total = kept[j] + in_buf[j].astype(jnp.float32)
        resid[:, first : first + part] = (base + total).astype(jnp.bfloat16)
    for j in range(parts):
        exchange(j).wait_send()
    for d in range(1, zn):
        relay(d, z).wait_send()

    for s in STREAMS:

        @pl.loop(1, n)
        def _(t):
            hop(s, t).wait_send()

        @pl.loop(0, n)
        def _(t):
            share(s, t).wait_send()

    swap_feat.wait_send()
    for copy in tail_out:
        copy.wait_send()


def scan_block(acc, halo, conv_w, bias, rates, ends, carry_s, z, g, cut, cols, seg):
    w = [conv_w[k : k + 1, :] for k in range(KERNEL)]
    b0, b1 = bias[0:1, :], bias[1:2, :]
    scale = -8.0 * rates
    row = lax.broadcasted_iota(jnp.int32, (SUB, cols), 0)

    def at(t):
        return pl.ds(pl.multiple_of((g * seg + t) * SUB, SUB), SUB)

    def before(j):
        rolled = pltpu.roll(acc[1, at(seg - j), cut], 1, 0)
        return jnp.where(row == 0, halo[KERNEL - 1 - j : KERNEL - j, :], rolled)

    def step(t, state):
        h, p, x1, x2, x3 = state
        here = at(t)
        x0 = acc[1, here, cut]
        conv = w[0] * x0 + w[1] * x1 + w[2] * x2 + w[3] * x3
        recur = jax.nn.sigmoid(acc[2, here, cut] + b0)
        inflow = jax.nn.sigmoid(acc[3, here, cut] + b1)
        a = jnp.exp(recur * scale)
        h = a * h + jnp.sqrt(1.0 - a * a) * inflow * conv
        p = a * p
        acc[0, here, cut] = jax.nn.gelu(acc[0, here, cut])
        acc[2, here, cut] = h
        acc[3, here, cut] = p
        return h, p, x0, x1, x2

    zero = jnp.zeros((SUB, cols), jnp.float32)
    h, p, _, _, _ = lax.fori_loop(
        0, seg, step, (zero, zero + 1.0, before(1), before(2), before(3)), unroll=4
    )
    run, dec = jnp.zeros((1, cols), jnp.float32), jnp.ones((1, cols), jnp.float32)
    for s in range(SUB):
        carry_s[0, s : s + 1, :] = run
        carry_s[1, s : s + 1, :] = dec
        run = p[s : s + 1] * run + h[s : s + 1]
        dec = p[s : s + 1] * dec
    ends[z, g, 0:1, cut] = run
    ends[z, g, 1:2, cut] = dec
    run, dec = carry_s[0], carry_s[1]

    def finish(t, _):
        here = at(t)
        gate, p = acc[0, here, cut], acc[3, here, cut]
        acc[2, here, cut] = (acc[2, here, cut] + p * run) * gate
        acc[3, here, cut] = p * dec * gate
        return 0

    lax.fori_loop(0, seg, finish, 0, unroll=4)


def core_block(emb, wb, wd, tail, conv_w, bias, rates, games):
    count, half = emb.shape
    rows, chans = wd.shape
    yn = lax.axis_size("width")
    n = lax.axis_size("tm") * (lax.axis_size("batch") // 2)
    depth = yn * half
    vmem = pl.BlockSpec(memory_space=pltpu.VMEM)
    hbm = pl.BlockSpec(memory_space=pl.ANY)
    dma = pltpu.SemaphoreType.DMA
    streams = len(STREAMS)
    zn = lax.axis_size("tm")
    own_rows = count // yn
    part = min(512, half)
    parts = depth // part
    return pl.pallas_call(
        core_kernel,
        in_specs=[hbm] * 4 + [vmem] * 3,
        out_specs=vmem,
        out_shape=jax.ShapeDtypeStruct((own_rows, depth), jnp.bfloat16),
        scratch_shapes=[
            pltpu.VMEM((4, depth, chans), jnp.bfloat16),
            pltpu.VMEM((4, count, chans), jnp.float32),
            pltpu.VMEM((3, games * SUB, half), jnp.bfloat16),
            pltpu.VMEM((games * SUB, chans), jnp.float32),
            pltpu.VMEM((2, SUB, min(512, chans)), jnp.float32),
            pltpu.VMEM((depth, chans), jnp.bfloat16),
            pltpu.VMEM((yn, count, half), jnp.bfloat16),
            pltpu.VMEM((zn, games, 2, chans), jnp.float32),
            pltpu.VMEM((games, chans), jnp.float32),
            pltpu.VMEM((count, chans), jnp.bfloat16),
            pltpu.VMEM((parts, own_rows, part), jnp.bfloat16),
            pltpu.VMEM((parts, own_rows, part), jnp.bfloat16),
            pltpu.VMEM((parts, own_rows, part), jnp.float32),
            dma((4,)), dma, dma, dma((2,)), dma((2,)),
            dma((streams, n)), dma((streams, n)), dma((streams, n)), dma((streams, n)),
            dma((zn,)), dma((zn,)), dma((parts,)), dma((parts,)),
        ],
        compiler_params=pltpu.CompilerParams(
            collective_id=0, has_side_effects=True, vmem_limit_bytes=56 * 1024 * 1024
        ),
        cost_estimate=pl.CostEstimate(
            flops=8 * count * chans * depth, bytes_accessed=200_000_000, transcendentals=8 * count * chans
        ),
    )(emb, wb, wd, tail, conv_w, bias, rates.reshape(1, chans))


def shards(
    moves,
    lengths,
    outcomes,
    embedded,
    w_branches,
    conv_w,
    gate_bias,
    rates,
    w_down,
    w_policy,
    w_value,
):
    games, block_len, half = embedded.shape
    count = games * block_len
    n_width = lax.axis_size("width")
    me = lax.axis_index("width")
    own_rows = count // n_width

    flat = interleave(embedded).reshape(count, half)
    heads = jnp.concatenate([w_policy, w_value[:, None]], 1)
    heads = both(heads, swap(heads, "width"), "width", 0)
    depth = n_width * half
    tail = flat.reshape(games, block_len // SUB, SUB, half)[:, 1 - KERNEL :, SUB - 1, :]
    tail = jnp.pad(tail, ((0, 0), (0, SUB + 1 - KERNEL), (0, 0))).reshape(games * SUB, half)
    resid = core_block(flat, w_branches, w_down, tail, conv_w, gate_bias, rates, games)
    here = lax.axis_index("tm")

    def mine(x):
        return lax.dynamic_slice_in_dim(x, me * own_rows, own_rows, 0)

    wide = resid.astype(jnp.float32)
    sumsq = jnp.sum(wide * wide, -1)
    scores = jnp.dot(resid, heads, preferred_element_type=jnp.float32)
    norm = lax.rsqrt(sumsq / depth + 1e-06)
    scores = scores * norm[:, None]
    logits = scores[:, :-1]
    value = jnp.tanh(scores[:, -1])
    top = jnp.max(logits, -1, keepdims=True)
    lse = top[:, 0] + jnp.log(jnp.sum(jnp.exp(logits - top), -1))
    column = lax.broadcasted_iota(jnp.int32, logits.shape, 1)
    picked = jnp.sum(jnp.where(column == mine(interleave(moves).reshape(count, 1)), logits, 0.0), -1)
    target = jnp.broadcast_to(outcomes.astype(jnp.float32)[:, None], (games, block_len))
    position = here * block_len + lax.broadcasted_iota(jnp.int32, (games, block_len), 1)
    live = interleave(position < lengths[:, None]).reshape(count)
    loss = jnp.where(mine(live), lse - picked + (value - mine(target.reshape(count))) ** 2, 0.0)
    result = jnp.stack([loss, value])
    result = both(result, swap(result, "width"), "width", 1)
    result = result.reshape(2, games, block_len)
    return (restore(result[0]), restore(result[1]))


def solution(mesh):
    in_specs = (
        P("batch", "tm"),
        P("batch"),
        P("batch"),
        P("batch", "tm", "width"),
        P(None, ("tm", "batch"), "width"),
        P(None, "width"),
        P(None, "width"),
        P("width"),
        P(("tm", "batch"), "width"),
        P("width", None),
        P("width"),
    )
    out_specs = (P("batch", "tm"), P("batch", "tm"))
    return jax.shard_map(shards, mesh=mesh, in_specs=in_specs, out_specs=out_specs, check_vma=False)
```

```python
import jax
import jax.numpy as jnp
from jax import lax
from jax.experimental import pallas as pl
from jax.experimental.pallas import tpu as pltpu
from jax.sharding import PartitionSpec as P

KERNEL = 4
SUB = 8
MESH = pl.DeviceIdType.MESH
STREAMS = tuple(range(6))
LAG = 2


def swap(value, axis):
    n = lax.axis_size(axis)
    return lax.ppermute(value, axis, [(i, n - 1 - i) for i in range(n)])


def interleave(x):
    games, steps = x.shape[:2]
    return jnp.swapaxes(x.reshape(games, SUB, steps // SUB, *x.shape[2:]), 1, 2).reshape(x.shape)


def restore(x):
    games, steps = x.shape[:2]
    return jnp.swapaxes(x.reshape(games, steps // SUB, SUB, *x.shape[2:]), 1, 2).reshape(x.shape)


def both(own, other, axis, dim):
    first = lax.axis_index(axis) == 0
    return jnp.concatenate([jnp.where(first, own, other), jnp.where(first, other, own)], dim)


def core_kernel(
    emb, wb, wd, tail, conv_w, bias, rates,
    resid,
    w_all, acc, tails, halo, carry_s, wd_all, feat, ends, state, mixed, out_buf, in_buf, kept,
    loc, feat_s, feat_r, tail_s, tail_r, ring_s, ring_r, peer_s, peer_r, ends_s, ends_r, out_s, out_r,
):
    z, b, y = lax.axis_index("tm"), lax.axis_index("batch"), lax.axis_index("width")
    zn, bn, yn = lax.axis_size("tm"), lax.axis_size("batch"), lax.axis_size("width")
    x, core = b // 2, b % 2
    n = zn * (bn // 2)
    rows, chans = wd.shape
    count, half = emb.shape
    games = ends.shape[1]
    width_cut = chans // 2

    def spot(r):
        cx = r // zn
        cz = r % zn
        return cz + (cx % 2) * (zn - 1 - 2 * cz), cx

    r = x * zn + z + (x % 2) * (zn - 1 - 2 * z)

    def at(place, c=core, w=y):
        return {"tm": place[0], "batch": place[1] * 2 + c, "width": w}

    ahead, behind = at(spot((r + 1) % n)), at(spot((r + n - 1) % n))
    peer = at((z, x), 1 - core)
    partner = at((z, x), core, yn - 1 - y)
    later, earlier = ((z + 1) % zn, x), ((z + zn - 1) % zn, x)
    tail_to = [at(later), at(later, core, yn - 1 - y)]
    greet = [ahead, behind, peer, partner] + tail_to + [at(earlier), at(earlier, core, yn - 1 - y)]
    greet += [at(((z + d) % zn, x)) for d in range(2, zn - 1)]

    def first_row(chip):
        cz, cx = spot(chip)
        return (cz * bn + cx * 2) * rows

    own = first_row(r) + core * rows
    own = pl.multiple_of(own, rows)
    local = [
        pltpu.make_async_copy(wb, w_all.at[:, pl.ds(own, rows), :], loc.at[0]),
        pltpu.make_async_copy(wd, wd_all.at[pl.ds(own, rows), :], loc.at[1]),
        pltpu.make_async_copy(emb, feat.at[y], loc.at[2]),
        pltpu.make_async_copy(tail, tails.at[2], loc.at[3]),
    ]
    for copy in local:
        copy.start()
    barrier = pltpu.get_barrier_semaphore()
    for device in greet:
        pl.semaphore_signal(barrier, inc=1, device_id=device, device_id_type=MESH)
    pl.semaphore_wait(barrier, len(greet))
    for copy in local:
        copy.wait()

    def remote(src, dst, send, recv, device):
        return pltpu.make_async_remote_copy(
            src_ref=src, dst_ref=dst, send_sem=send, recv_sem=recv, device_id=device, device_id_type=MESH
        )

    def forward(s):
        return s in (0, 1, 4)

    def chip_of(s, t):
        return (r + n - t) % n if forward(s) else (r + t) % n

    def piece(s, chip, c):
        at_row = pl.ds(pl.multiple_of(first_row(chip) + c * rows, rows), rows)
        if s < 4:
            return w_all.at[s, at_row, :]
        return wd_all.at[at_row, pl.ds((s - 4) * width_cut, width_cut)]

    def hop(s, t):
        ref = piece(s, chip_of(s, t - 1), core)
        return remote(ref, ref, ring_s.at[s, t], ring_r.at[s, t], ahead if forward(s) else behind)

    def landed(s, t):
        ref = piece(s, chip_of(s, t), core)
        return remote(ref, ref, ring_s.at[s, t], ring_r.at[s, t], ahead if forward(s) else behind)

    def share(s, t):
        ref = piece(s, chip_of(s, t), core)
        return remote(ref, ref, peer_s.at[s, t], peer_r.at[s, t], peer)

    def shared(s, t):
        ref = piece(s, chip_of(s, t), 1 - core)
        return remote(ref, ref, peer_s.at[s, t], peer_r.at[s, t], peer)

    for s in STREAMS[:4]:
        hop(s, 1).start()
    swap_feat = remote(feat.at[y], feat.at[y], feat_s, feat_r, partner)
    swap_feat.start()
    tail_out = [
        remote(tails.at[2], tails.at[y], tail_s.at[i], tail_r.at[i], tail_to[i]) for i in range(2)
    ]
    for copy in tail_out:
        copy.start()
    for s in STREAMS:
        share(s, 0).start()
    acc[...] = jnp.zeros_like(acc)
    ref = feat.at[yn - 1 - y]
    remote(ref, ref, feat_s, feat_r, partner).wait_recv()

    tile = min(512, chans)
    eager = (2 * rows) % 128 == 0

    def product(s, start, depth):
        owner, col = start // half, pl.multiple_of(start % half, depth)
        left = feat[owner, :, pl.ds(col, depth)]

        @pl.loop(0, chans // tile)
        def _(j):
            cut = pl.ds(pl.multiple_of(j * tile, tile), tile)
            acc[s, :, cut] += jnp.dot(
                left,
                w_all[s, pl.ds(pl.multiple_of(start, depth), depth), cut],
                preferred_element_type=jnp.float32,
            )

    def compute(t):
        for s in STREAMS[:4]:
            shared(s, t).wait_recv()
            if eager:
                product(s, first_row(chip_of(s, t)), 2 * rows)

    def pump(s, t):
        landed(s, t).wait_recv()

        @pl.when(t < n - 1)
        def _():
            hop(s, t + 1).start()

        share(s, t).start()

    @pl.loop(1, n)
    def _(t):
        for s in STREAMS[:4]:
            pump(s, t)
        for s in STREAMS[4:]:

            @pl.when(t == LAG)
            def _():
                hop(s, 1).start()

            @pl.when(t > LAG)
            def _():
                pump(s, t - LAG)

        compute(t - 1)

    compute(n - 1)
    if not eager:
        depth = min(256, half)

        @pl.loop(0, yn * half // depth)
        def _(i):
            for s in range(4):
                product(s, i * depth, depth)

    for i in range(2):
        ref = tails.at[y if i == 0 else yn - 1 - y]
        remote(ref, ref, tail_s.at[i], tail_r.at[i], tail_to[i]).wait_recv()
    cols = min(512, chans)
    blocks = chans // cols

    @pl.loop(0, blocks)
    def _(j):
        cut = pl.ds(pl.multiple_of(j * cols, cols), cols)
        edge = jnp.zeros((tails.shape[1], cols), jnp.float32)
        for owner in range(yn):
            edge += jnp.dot(
                tails[owner],
                w_all[1, owner * half : (owner + 1) * half, cut],
                preferred_element_type=jnp.float32,
            )
        halo[:, cut] = jnp.where(z > 0, edge, 0.0)

    steps = count // games
    seg = steps // SUB

    @pl.loop(0, games * blocks)
    def _(u):
        g, j = u // blocks, u % blocks
        for s in STREAMS[4:]:

            @pl.when(u == 0)
            def _():
                pump(s, n - 2)

            @pl.when(u == games * blocks - 1)
            def _():
                pump(s, n - 1)

        cut = pl.ds(pl.multiple_of(j * cols, cols), cols)
        scan_block(
            acc, halo[pl.ds(pl.multiple_of(g * SUB, SUB), SUB), cut], conv_w[:, cut], bias[:, cut], rates[:, cut],
            ends, carry_s, z, g, cut, cols, seg,
        )

    def relay(d, source):
        ref = ends.at[source]
        return remote(ref, ref, ends_s.at[d], ends_r.at[d], at(((z + d) % zn, x)))

    for d in range(1, zn):
        relay(d, z).start()
    for d in range(1, zn):
        relay(d, (z + zn - d) % zn).wait_recv()
    for g in range(games):
        run = jnp.zeros((1, chans), jnp.float32)
        for j in range(zn - 1):
            run = jnp.where(j < z, ends[j, g, 1:2, :] * run + ends[j, g, 0:1, :], run)
        state[g : g + 1, :] = run
    for g in range(games):
        run = state[g : g + 1, :]

        @pl.loop(0, steps // 16)
        def _(i):
            here = pl.ds(pl.multiple_of(g * steps + i * 16, 16), 16)
            mixed[here, :] = (acc[2, here, :] + acc[3, here, :] * run).astype(jnp.bfloat16)

    for s in STREAMS[4:]:

        @pl.loop(0, n)
        def _(t):
            shared(s, t).wait_recv()

    parts, own_rows, part = out_buf.shape
    mine = pl.ds(pl.multiple_of(y * own_rows, own_rows), own_rows)
    theirs = pl.ds(pl.multiple_of((yn - 1 - y) * own_rows, own_rows), own_rows)

    def down(which, j):
        return lax.dot_general(
            mixed[which, :],
            wd_all[j * part : (j + 1) * part, :],
            (((1,), (1,)), ((), ())),
            preferred_element_type=jnp.float32,
        )

    def exchange(j):
        return remote(out_buf.at[j], in_buf.at[j], out_s.at[j], out_r.at[j], partner)

    for j in range(parts):
        out_buf[j] = down(theirs, j).astype(jnp.bfloat16)
        if j:
            exchange(j - 1).start()
    kept[0] = down(mine, 0)
    exchange(parts - 1).start()
    for j in range(1, parts):
        kept[j] = down(mine, j)
    for j in range(parts):
        exchange(j).wait_recv()
        first = j * part
        base = feat[first // half, mine, first % half : first % half + part].astype(jnp.float32)
        total = kept[j] + in_buf[j].astype(jnp.float32)
        resid[:, first : first + part] = (base + total).astype(jnp.bfloat16)
    for j in range(parts):
        exchange(j).wait_send()
    for d in range(1, zn):
        relay(d, z).wait_send()

    for s in STREAMS:

        @pl.loop(1, n)
        def _(t):
            hop(s, t).wait_send()

        @pl.loop(0, n)
        def _(t):
            share(s, t).wait_send()

    swap_feat.wait_send()
    for copy in tail_out:
        copy.wait_send()


def scan_block(acc, halo, conv_w, bias, rates, ends, carry_s, z, g, cut, cols, seg):
    w = [conv_w[k : k + 1, :] for k in range(KERNEL)]
    b0, b1 = bias[0:1, :], bias[1:2, :]
    scale = -8.0 * rates
    row = lax.broadcasted_iota(jnp.int32, (SUB, cols), 0)

    def at(t):
        return pl.ds(pl.multiple_of((g * seg + t) * SUB, SUB), SUB)

    def before(j):
        rolled = pltpu.roll(acc[1, at(seg - j), cut], 1, 0)
        return jnp.where(row == 0, halo[KERNEL - 1 - j : KERNEL - j, :], rolled)

    def step(t, state):
        h, p, x1, x2, x3 = state
        here = at(t)
        x0 = acc[1, here, cut]
        conv = w[0] * x0 + w[1] * x1 + w[2] * x2 + w[3] * x3
        recur = jax.nn.sigmoid(acc[2, here, cut] + b0)
        inflow = jax.nn.sigmoid(acc[3, here, cut] + b1)
        a = jnp.exp(recur * scale)
        h = a * h + jnp.sqrt(1.0 - a * a) * inflow * conv
        p = a * p
        acc[0, here, cut] = jax.nn.gelu(acc[0, here, cut])
        acc[2, here, cut] = h
        acc[3, here, cut] = p
        return h, p, x0, x1, x2

    zero = jnp.zeros((SUB, cols), jnp.float32)
    h, p, _, _, _ = lax.fori_loop(
        0, seg, step, (zero, zero + 1.0, before(1), before(2), before(3)), unroll=4
    )
    run, dec = jnp.zeros((1, cols), jnp.float32), jnp.ones((1, cols), jnp.float32)
    for s in range(SUB):
        carry_s[0, s : s + 1, :] = run
        carry_s[1, s : s + 1, :] = dec
        run = p[s : s + 1] * run + h[s : s + 1]
        dec = p[s : s + 1] * dec
    ends[z, g, 0:1, cut] = run
    ends[z, g, 1:2, cut] = dec
    run, dec = carry_s[0], carry_s[1]

    def finish(t, _):
        here = at(t)
        gate, p = acc[0, here, cut], acc[3, here, cut]
        acc[2, here, cut] = (acc[2, here, cut] + p * run) * gate
        acc[3, here, cut] = p * dec * gate
        return 0

    lax.fori_loop(0, seg, finish, 0, unroll=4)


def core_block(emb, wb, wd, tail, conv_w, bias, rates, games):
    count, half = emb.shape
    rows, chans = wd.shape
    yn = lax.axis_size("width")
    n = lax.axis_size("tm") * (lax.axis_size("batch") // 2)
    depth = yn * half
    vmem = pl.BlockSpec(memory_space=pltpu.VMEM)
    hbm = pl.BlockSpec(memory_space=pl.ANY)
    dma = pltpu.SemaphoreType.DMA
    streams = len(STREAMS)
    zn = lax.axis_size("tm")
    own_rows = count // yn
    part = min(512, half)
    parts = depth // part
    return pl.pallas_call(
        core_kernel,
        in_specs=[hbm] * 4 + [vmem] * 3,
        out_specs=vmem,
        out_shape=jax.ShapeDtypeStruct((own_rows, depth), jnp.bfloat16),
        scratch_shapes=[
            pltpu.VMEM((4, depth, chans), jnp.bfloat16),
            pltpu.VMEM((4, count, chans), jnp.float32),
            pltpu.VMEM((3, games * SUB, half), jnp.bfloat16),
            pltpu.VMEM((games * SUB, chans), jnp.float32),
            pltpu.VMEM((2, SUB, min(512, chans)), jnp.float32),
            pltpu.VMEM((depth, chans), jnp.bfloat16),
            pltpu.VMEM((yn, count, half), jnp.bfloat16),
            pltpu.VMEM((zn, games, 2, chans), jnp.float32),
            pltpu.VMEM((games, chans), jnp.float32),
            pltpu.VMEM((count, chans), jnp.bfloat16),
            pltpu.VMEM((parts, own_rows, part), jnp.bfloat16),
            pltpu.VMEM((parts, own_rows, part), jnp.bfloat16),
            pltpu.VMEM((parts, own_rows, part), jnp.float32),
            dma((4,)), dma, dma, dma((2,)), dma((2,)),
            dma((streams, n)), dma((streams, n)), dma((streams, n)), dma((streams, n)),
            dma((zn,)), dma((zn,)), dma((parts,)), dma((parts,)),
        ],
        compiler_params=pltpu.CompilerParams(
            collective_id=0, has_side_effects=True, vmem_limit_bytes=56 * 1024 * 1024
        ),
        cost_estimate=pl.CostEstimate(
            flops=8 * count * chans * depth, bytes_accessed=200_000_000, transcendentals=8 * count * chans
        ),
    )(emb, wb, wd, tail, conv_w, bias, rates.reshape(1, chans))


def shards(
    moves,
    lengths,
    outcomes,
    embedded,
    w_branches,
    conv_w,
    gate_bias,
    rates,
    w_down,
    w_policy,
    w_value,
):
    games, block_len, half = embedded.shape
    count = games * block_len
    n_width = lax.axis_size("width")
    me = lax.axis_index("width")
    own_rows = count // n_width

    flat = interleave(embedded).reshape(count, half)
    heads = jnp.concatenate([w_policy, w_value[:, None]], 1)
    heads = both(heads, swap(heads, "width"), "width", 0)
    depth = n_width * half
    tail = flat.reshape(games, block_len // SUB, SUB, half)[:, 1 - KERNEL :, SUB - 1, :]
    tail = jnp.pad(tail, ((0, 0), (0, SUB + 1 - KERNEL), (0, 0))).reshape(games * SUB, half)
    resid = core_block(flat, w_branches, w_down, tail, conv_w, gate_bias, rates, games)
    here = lax.axis_index("tm")

    def mine(x):
        return lax.dynamic_slice_in_dim(x, me * own_rows, own_rows, 0)

    wide = resid.astype(jnp.float32)
    sumsq = jnp.sum(wide * wide, -1)
    scores = jnp.dot(resid, heads, preferred_element_type=jnp.float32)
    norm = lax.rsqrt(sumsq / depth + 1e-06)
    scores = scores * norm[:, None]
    logits = scores[:, :-1]
    value = jnp.tanh(scores[:, -1])
    top = jnp.max(logits, -1, keepdims=True)
    lse = top[:, 0] + jnp.log(jnp.sum(jnp.exp(logits - top), -1))
    column = lax.broadcasted_iota(jnp.int32, logits.shape, 1)
    picked = jnp.sum(jnp.where(column == mine(interleave(moves).reshape(count, 1)), logits, 0.0), -1)
    target = jnp.broadcast_to(outcomes.astype(jnp.float32)[:, None], (games, block_len))
    position = here * block_len + lax.broadcasted_iota(jnp.int32, (games, block_len), 1)
    live = interleave(position < lengths[:, None]).reshape(count)
    loss = jnp.where(mine(live), lse - picked + (value - mine(target.reshape(count))) ** 2, 0.0)
    result = jnp.stack([loss, value])
    result = both(result, swap(result, "width"), "width", 1)
    result = result.reshape(2, games, block_len)
    return (restore(result[0]), restore(result[1]))


def solution(mesh):
    in_specs = (
        P("batch", "tm"),
        P("batch"),
        P("batch"),
        P("batch", "tm", "width"),
        P(None, ("tm", "batch"), "width"),
        P(None, "width"),
        P(None, "width"),
        P("width"),
        P(("tm", "batch"), "width"),
        P("width", None),
        P("width"),
    )
    out_specs = (P("batch", "tm"), P("batch", "tm"))
    return jax.shard_map(shards, mesh=mesh, in_specs=in_specs, out_specs=out_specs, check_vma=False)
```
